8 devices in a mesh: rep: 1 (over z), heads: 2 (over y), pool: 4 (over x, core).
Axes of the slice: x: 2, y: 2, z: 1, core: 2. Of those that a mesh axis runs over, the one named last changes fastest.
Arguments:
- kv_pool: bfloat16 [2, 512, 2, 32, 8, 128], P(None, ('rep', 'pool'), None, None, 'heads')
- page_idx: int32 [4, 4, 4], P('rep', 'pool')
- x_tokens: bfloat16 [4, 256, 5120], P(('rep', 'pool'))
- gain_attn: bfloat16 [2, 5120], replicated
- w_q: bfloat16 [2, 5120, 5120], P(None, None, 'heads')
- w_k: bfloat16 [2, 5120, 1024], P(None, None, 'heads')
- w_v: bfloat16 [2, 5120, 1024], P(None, None, 'heads')
- w_o: bfloat16 [2, 5120, 5120], P(None, 'heads')
- gain_mlp: bfloat16 [2, 5120], replicated
- w_gate: bfloat16 [2, 5120, 13824], P(None, None, 'heads')
- w_up: bfloat16 [2, 5120, 13824], P(None, None, 'heads')
- w_down: bfloat16 [2, 13824, 5120], P(None, 'heads')
Outputs:
- output: bfloat16 [4, 256, 5120], P(('rep', 'pool'))
All inputs are finite; a program needn't handle non-finite values.
Results may differ from the reference program's by a relative error of at most 0.02.
Values are sent between devices in bfloat16 or wider.
A program may use at most 2.25 GiB of HBM per device.

```python
import jax
import jax.numpy as jnp
from jax import lax

LAYERS = 2
OWNERS = 4
POOL_PAGES = 128
REQ_PAGES = 4
PAGE_LEN = 32
KV_HEADS = 8
HEAD_DIM = 128
TOKENS = 256
D_MODEL = 5120
Q_HEADS = 40
FFN_DIM = 13824

PREFIX = OWNERS * REQ_PAGES * PAGE_LEN
GROUP_Q = Q_HEADS // KV_HEADS


def setup_inputs(seed: int = 0, part: int = 0) -> dict:
    shared_keys = jax.random.split(jax.random.key(seed), 10)
    part_keys = jax.random.split(jax.random.fold_in(jax.random.key(seed + 1), part), 3)
    pool_shape = (LAYERS, OWNERS * POOL_PAGES, 2, PAGE_LEN, KV_HEADS, HEAD_DIM)
    kv_pool = (2.0 * jax.random.normal(part_keys[0], pool_shape, jnp.float32)).astype(jnp.bfloat16)
    pick_keys = jax.random.split(part_keys[1], OWNERS * OWNERS)
    page_idx = jax.vmap(lambda one_key: jax.random.permutation(one_key, POOL_PAGES)[:REQ_PAGES])(pick_keys)
    page_idx = page_idx.reshape(OWNERS, OWNERS, REQ_PAGES).astype(jnp.int32)
    x_tokens = (0.5 * jax.random.normal(part_keys[2], (OWNERS, TOKENS, D_MODEL), jnp.float32)).astype(jnp.bfloat16)

    def draw_weight(w_key, arr_shape, fan_in):
        return (jax.random.normal(w_key, arr_shape, jnp.float32) * fan_in ** -0.5).astype(jnp.bfloat16)

    def draw_gains(g_key):
        return (1.0 + 0.3 * jax.random.normal(g_key, (LAYERS, D_MODEL), jnp.float32)).astype(jnp.bfloat16)

    q_width = Q_HEADS * HEAD_DIM
    kv_width = KV_HEADS * HEAD_DIM
    return {
        'kv_pool': kv_pool,
        'page_idx': page_idx,
        'x_tokens': x_tokens,
        'gain_attn': draw_gains(shared_keys[0]),
        'w_q': draw_weight(shared_keys[1], (LAYERS, D_MODEL, q_width), D_MODEL),
        'w_k': draw_weight(shared_keys[2], (LAYERS, D_MODEL, kv_width), D_MODEL / 4.0),
        'w_v': draw_weight(shared_keys[3], (LAYERS, D_MODEL, kv_width), D_MODEL / 4.0),
        'w_o': draw_weight(shared_keys[4], (LAYERS, q_width, D_MODEL), q_width),
        'gain_mlp': draw_gains(shared_keys[5]),
        'w_gate': draw_weight(shared_keys[6], (LAYERS, D_MODEL, FFN_DIM), D_MODEL),
        'w_up': draw_weight(shared_keys[7], (LAYERS, D_MODEL, FFN_DIM), D_MODEL),
        'w_down': draw_weight(shared_keys[8], (LAYERS, FFN_DIM, D_MODEL), FFN_DIM),
    }


def rms_norm(hidden, gain_vec):
    hid_f32 = hidden.astype(jnp.float32)
    inv_rms = lax.rsqrt(jnp.mean(hid_f32 * hid_f32, axis=-1, keepdims=True) + 1e-5)
    return (hid_f32 * inv_rms * gain_vec.astype(jnp.float32)).astype(jnp.bfloat16)


def rope_tables():
    positions = (PREFIX + jnp.arange(TOKENS)).astype(jnp.float32)
    inv_freq = 10000.0 ** (-2.0 * jnp.arange(HEAD_DIM // 2).astype(jnp.float32) / HEAD_DIM)
    angles = positions[:, None] * inv_freq[None, :]
    return jnp.cos(angles)[:, None, :], jnp.sin(angles)[:, None, :]


def apply_rope(projected, cos_tab, sin_tab):
    half_dim = HEAD_DIM // 2
    first_half = projected[..., :half_dim]
    second_half = projected[..., half_dim:]
    return jnp.concatenate([first_half * cos_tab - second_half * sin_tab, second_half * cos_tab + first_half * sin_tab], axis=-1)


def reference(kv_pool, page_idx, x_tokens, gain_attn, w_q, w_k, w_v, w_o, gain_mlp, w_gate, w_up, w_down):
    cos_tab, sin_tab = rope_tables()
    owner_base = jnp.arange(OWNERS)[:, None] * POOL_PAGES
    allowed = jnp.arange(PREFIX + TOKENS)[None, :] <= PREFIX + jnp.arange(TOKENS)[:, None]

    def layer_step(hidden, layer_in):
        pool_layer, gain_a, wq_layer, wk_layer, wv_layer, wo_layer, gain_m, wg_layer, wu_layer, wd_layer = layer_in
        h_att = rms_norm(hidden, gain_a).reshape(OWNERS * TOKENS, D_MODEL)
        q_proj = jnp.dot(h_att, wq_layer, preferred_element_type=jnp.float32).reshape(OWNERS, TOKENS, Q_HEADS, HEAD_DIM)
        k_proj = jnp.dot(h_att, wk_layer, preferred_element_type=jnp.float32).reshape(OWNERS, TOKENS, KV_HEADS, HEAD_DIM)
        queries = apply_rope(q_proj, cos_tab, sin_tab).astype(jnp.bfloat16)
        k_new = apply_rope(k_proj, cos_tab, sin_tab).astype(jnp.bfloat16)
        v_new = jnp.dot(h_att, wv_layer, preferred_element_type=jnp.float32).astype(jnp.bfloat16).reshape(OWNERS, TOKENS, KV_HEADS, HEAD_DIM)

        def one_request(per_req):
            q_req, k_req, v_req, idx_req = per_req
            page_rows = (owner_base + idx_req).reshape(OWNERS * REQ_PAGES)
            fetched = pool_layer[page_rows]
            key_all = jnp.concatenate([fetched[:, 0].reshape(PREFIX, KV_HEADS, HEAD_DIM), k_req], axis=0).astype(jnp.float32)
            val_all = jnp.concatenate([fetched[:, 1].reshape(PREFIX, KV_HEADS, HEAD_DIM), v_req], axis=0).astype(jnp.float32)
            q_grp = q_req.astype(jnp.float32).reshape(TOKENS, KV_HEADS, GROUP_Q, HEAD_DIM)
            scores = jnp.einsum('tgrd,ngd->grtn', q_grp, key_all) * HEAD_DIM ** -0.5
            scores = jnp.where(allowed, scores, -jnp.inf)
            probs_bf = jax.nn.softmax(scores, axis=-1).astype(jnp.bfloat16)
            attn_sum = jnp.einsum('grtn,ngd->tgrd', probs_bf.astype(jnp.float32), val_all)
            return attn_sum.reshape(TOKENS, Q_HEADS * HEAD_DIM).astype(jnp.bfloat16)

        attn_cat = lax.map(one_request, (queries, k_new, v_new, page_idx))
        attn_out = jnp.dot(attn_cat.reshape(OWNERS * TOKENS, Q_HEADS * HEAD_DIM), wo_layer, preferred_element_type=jnp.float32).reshape(OWNERS, TOKENS, D_MODEL)
        x_mid = (hidden.astype(jnp.float32) + attn_out).astype(jnp.bfloat16)
        h_mlp = rms_norm(x_mid, gain_m).reshape(OWNERS * TOKENS, D_MODEL)
        gate_proj = jnp.dot(h_mlp, wg_layer, preferred_element_type=jnp.float32)
        up_proj = jnp.dot(h_mlp, wu_layer, preferred_element_type=jnp.float32)
        act_out = (jax.nn.silu(gate_proj) * up_proj).astype(jnp.bfloat16)
        mlp_out = jnp.dot(act_out, wd_layer, preferred_element_type=jnp.float32).reshape(OWNERS, TOKENS, D_MODEL)
        return (x_mid.astype(jnp.float32) + mlp_out).astype(jnp.bfloat16), None

    x_out, _ = lax.scan(layer_step, x_tokens, (kv_pool, gain_attn, w_q, w_k, w_v, w_o, gain_mlp, w_gate, w_up, w_down))
    return x_out
```

```python
import functools

import jax
import jax.numpy as jnp
from jax import lax
from jax.experimental import pallas as pl
from jax.experimental.pallas import tpu as pltpu
from jax.sharding import PartitionSpec as P

MESH = pl.DeviceIdType.MESH
F32 = jnp.float32
BF16 = jnp.bfloat16
TILE = 256
SLOTS = 9
AHEAD = SLOTS - 1


def rope_tables(prefix, tokens, head_dim):
    positions = (prefix + jnp.arange(tokens)).astype(F32)
    inv_freq = 10000.0 ** (-2.0 * jnp.arange(head_dim // 2).astype(F32) / head_dim)
    angles = positions[:, None] * inv_freq[None, :]
    cos_tab, sin_tab = jnp.cos(angles), jnp.sin(angles)
    return jnp.concatenate([cos_tab, cos_tab], axis=-1), jnp.concatenate([-sin_tab, sin_tab], axis=-1)


def layers_kernel(
    dims,
    kv_hbm, x_hbm, cos_ref, sin_ref, ga_ref, gm_ref,
    wq_hbm, wk_hbm, wv_hbm, wo_hbm, wg_hbm, wu_hbm, wd_hbm,
    out_hbm,
    ring, xbuf, hbuf, qbuf, kbuf, vbuf, abuf, ubuf, pbuf, rbuf, kvbuf,
    ring_sem, load_sem, rs_send, rs_recv, ag_send, ag_recv,
):
    layers, tokens, kv_loc, group_q, head_dim, width, ffn, prefix = dims
    q_loc = kv_loc * group_q
    rows = tokens // 2
    half = rows // 2
    per_tile = TILE // head_dim
    scale = head_dim ** -0.5

    me = lax.axis_index('heads')
    other = 1 - me

    n_q, n_kv = q_loc * head_dim // TILE, kv_loc * head_dim // TILE
    n_d, n_f = width // TILE, ffn // TILE
    attn_seq = [('q', n_q), ('k', n_kv), ('v', n_kv), ('o', n_d)]
    mlp_seq = [('gu', 2 * n_f), ('d', n_d)]
    phases = attn_seq + attn_seq + mlp_seq + mlp_seq
    bases = [sum(n for _, n in phases[:p]) for p in range(len(phases))]
    per_layer = sum(n for _, n in phases)
    q_rows = q_loc * head_dim

    def copies(kind, layer, idx, slot):
        def tile(w_hbm, depth, col):
            start = col * TILE if isinstance(col, int) else pl.multiple_of(col * TILE, TILE)
            return pltpu.make_async_copy(w_hbm.at[layer, :, pl.ds(start, TILE)], ring.at[slot, pl.ds(0, depth), :], ring_sem.at[slot])
        if kind == 'q':
            return tile(wq_hbm, width, idx)
        if kind == 'k':
            return tile(wk_hbm, width, idx)
        if kind == 'v':
            return tile(wv_hbm, width, idx)
        if kind == 'o':
            return tile(wo_hbm, q_rows, idx)
        if kind == 'g':
            return tile(wg_hbm, width, idx)
        if kind == 'u':
            return tile(wu_hbm, width, idx)
        return tile(wd_hbm, ffn, idx)

    def start_tile(phase, layer, idx, slot):
        kind = phases[phase][0]
        if kind != 'gu':
            copies(kind, layer, idx, slot).start()
        elif isinstance(idx, int):
            copies('gu'[idx % 2], layer, idx // 2, slot).start()
        else:
            @pl.when(lax.rem(idx, 2) == 0)
            def _():
                copies('g', layer, idx // 2, slot).start()

            @pl.when(lax.rem(idx, 2) == 1)
            def _():
                copies('u', layer, idx // 2, slot).start()

    def prefetch(phase, layer, idx):
        slot = lax.rem(layer * per_layer + bases[phase] + idx + AHEAD, SLOTS)
        lo = -AHEAD
        p, wrapped = phase, False
        count = phases[phase][1]
        while lo < count:
            hi = lo + phases[p][1]
            if hi > 0:
                local = idx - lo
                cond = (idx >= lo) & (idx < hi)
                target = layer + 1 if wrapped else layer
                if wrapped:
                    cond = cond & (target < layers)

                @pl.when(cond)
                def _(p=p, target=target, local=local):
                    start_tile(p, target, local, slot)
            lo = hi
            p += 1
            if p == len(phases):
                p, wrapped = 0, True

    def take(phase, layer, idx, kind, col):
        prefetch(phase, layer, idx)
        slot = lax.rem(layer * per_layer + bases[phase] + idx, SLOTS)
        copies(kind, layer, col, slot).wait()
        return slot

    def norm(chunk, gain_ref, layer):
        step = 16

        def body(i, carry):
            at = pl.multiple_of(chunk * rows + i * step, step)
            to = pl.multiple_of(i * step, step)
            hid = xbuf[pl.ds(at, step), :].astype(F32)
            inv = lax.rsqrt(jnp.mean(hid * hid, axis=-1, keepdims=True) + 1e-5)
            hbuf[pl.ds(to, step), :] = (hid * inv * gain_ref[layer]).astype(BF16)
            return carry

        lax.fori_loop(0, rows // step, body, 0)

    def roped(block, chunk):
        cos = cos_ref[chunk * rows:(chunk + 1) * rows, :]
        sin = sin_ref[chunk * rows:(chunk + 1) * rows, :]
        return (block * cos + pltpu.roll(block, head_dim // 2, 1) * sin).astype(BF16)

    def project(phase, chunk, layer):
        def q_body(i, carry):
            slot = take(phase, layer, i, 'q', i)
            res = jnp.dot(hbuf[...], ring[slot, :width, :], preferred_element_type=F32)
            for s in range(per_tile):
                qbuf[i * per_tile + s] = roped(res[:, s * head_dim:(s + 1) * head_dim], chunk)
            return carry

        def k_body(i, carry):
            slot = take(phase + 1, layer, i, 'k', i)
            res = jnp.dot(hbuf[...], ring[slot, :width, :], preferred_element_type=F32)
            for s in range(per_tile):
                kbuf[i * per_tile + s, chunk * rows:(chunk + 1) * rows, :] = roped(res[:, s * head_dim:(s + 1) * head_dim], chunk)
            return carry

        def v_body(i, carry):
            slot = take(phase + 2, layer, i, 'v', i)
            res = jnp.dot(hbuf[...], ring[slot, :width, :], preferred_element_type=F32)
            for s in range(per_tile):
                vbuf[i * per_tile + s, chunk * rows:(chunk + 1) * rows, :] = res[:, s * head_dim:(s + 1) * head_dim].astype(BF16)
            return carry

        lax.fori_loop(0, n_q, q_body, 0)
        lax.fori_loop(0, n_kv, k_body, 0)
        lax.fori_loop(0, n_kv, v_body, 0)

    def attend(chunk, layer):
        n_new = (chunk + 1) * rows
        nt = (((1,), (1,)), ((), ()))

        def body(g, carry):
            for r in range(group_q):
                q = qbuf[g * group_q + r]
                s_pre = lax.dot_general(q, kvbuf[layer, 0, g], nt, preferred_element_type=F32) * scale
                s_new = lax.dot_general(q, kbuf[g, :n_new, :], nt, preferred_element_type=F32) * scale
                tok = chunk * rows + lax.broadcasted_iota(jnp.int32, (rows, n_new), 0)
                key = lax.broadcasted_iota(jnp.int32, (rows, n_new), 1)
                s_new = jnp.where(key <= tok, s_new, -jnp.inf)
                top = jnp.maximum(jnp.max(s_pre, axis=-1, keepdims=True), jnp.max(s_new, axis=-1, keepdims=True))
                e_pre = jnp.exp(s_pre - top)
                e_new = jnp.exp(s_new - top)
                inv = 1.0 / (jnp.sum(e_pre, axis=-1, keepdims=True) + jnp.sum(e_new, axis=-1, keepdims=True))
                att = jnp.dot((e_pre * inv).astype(BF16), kvbuf[layer, 1, g], preferred_element_type=F32)
                att = att + jnp.dot((e_new * inv).astype(BF16), vbuf[g, :n_new, :], preferred_element_type=F32)
                col = pl.multiple_of((g * group_q + r) * head_dim, head_dim)
                abuf[:, pl.ds(col, head_dim)] = att.astype(BF16)
            return carry

        lax.fori_loop(0, kv_loc, body, 0)

    def send_block(chunk, col, cols):
        at = pl.multiple_of(other * half, half)
        return pltpu.make_async_remote_copy(
            src_ref=pbuf.at[chunk, pl.ds(at, half), pl.ds(col, cols)],
            dst_ref=rbuf.at[chunk, :, pl.ds(col, cols)],
            send_sem=rs_send.at[chunk],
            recv_sem=rs_recv.at[chunk],
            device_id={'heads': other},
            device_id_type=MESH,
        )

    def reduce_out(phase, chunk, layer, kind, src, depth):
        def body(i, carry):
            slot = take(phase, layer, i, kind, i)
            res = jnp.dot(src[...], ring[slot, :depth, :], preferred_element_type=F32)
            pbuf[chunk, :, pl.ds(pl.multiple_of(i * TILE, TILE), TILE)] = res

            @pl.when(i > 0)
            def _():
                send_block(chunk, pl.multiple_of((i - 1) * TILE, TILE), TILE).start()
            return carry

        lax.fori_loop(0, n_d, body, 0)
        send_block(chunk, width - TILE, TILE).start()

    def share(chunk):
        at = pl.multiple_of(chunk * rows + me * half, half)
        return pltpu.make_async_remote_copy(
            src_ref=xbuf.at[pl.ds(at, half), :],
            dst_ref=xbuf.at[pl.ds(at, half), :],
            send_sem=ag_send.at[chunk],
            recv_sem=ag_recv.at[chunk],
            device_id={'heads': other},
            device_id_type=MESH,
        )

    def reduce_and_share(chunk):
        whole = send_block(chunk, 0, width)
        whole.wait_recv()
        step = 16

        def body(i, carry):
            at = pl.multiple_of(chunk * rows + me * half + i * step, step)
            mine = pl.multiple_of(me * half + i * step, step)
            got = pl.multiple_of(i * step, step)
            total = pbuf[chunk, pl.ds(mine, step), :] + rbuf[chunk, pl.ds(got, step), :]
            xbuf[pl.ds(at, step), :] = (xbuf[pl.ds(at, step), :].astype(F32) + total).astype(BF16)
            return carry

        lax.fori_loop(0, half // step, body, 0)
        whole.wait_send()
        share(chunk).start()

    def shared(chunk):
        share(chunk).wait()

    def gate_up(phase, layer, first, last):
        def body(i, carry):
            slot = take(phase, layer, 2 * i, 'g', i)
            gate = jnp.dot(hbuf[...], ring[slot, :width, :], preferred_element_type=F32)
            slot = take(phase, layer, 2 * i + 1, 'u', i)
            up = jnp.dot(hbuf[...], ring[slot, :width, :], preferred_element_type=F32)
            ubuf[:, pl.ds(pl.multiple_of(i * TILE, TILE), TILE)] = (jax.nn.silu(gate) * up).astype(BF16)
            return carry

        lax.fori_loop(first, last, body, 0)

    for g in range(AHEAD):
        p = max(k for k in range(len(phases)) if bases[k] <= g)
        start_tile(p, 0, g - bases[p], g)
    x_load = pltpu.make_async_copy(x_hbm, xbuf, load_sem.at[0])
    kv_load = pltpu.make_async_copy(kv_hbm, kvbuf, load_sem.at[1])
    x_load.start()
    kv_load.start()

    barrier = pltpu.get_barrier_semaphore()
    pl.semaphore_signal(barrier, inc=1, device_id={'heads': other}, device_id_type=MESH)
    pl.semaphore_wait(barrier, 1)

    x_load.wait()
    kv_load.wait()

    a_cut = min(n_f, 20)
    b_cut = min(n_f, 10)

    def layer_body(layer, carry):
        @pl.when(layer > 0)
        def _():
            shared(0)
        norm(0, ga_ref, layer)
        project(0, 0, layer)

        @pl.when(layer > 0)
        def _():
            reduce_and_share(1)
        attend(0, layer)
        reduce_out(3, 0, layer, 'o', abuf, q_rows)

        @pl.when(layer > 0)
        def _():
            shared(1)
        norm(1, ga_ref, layer)
        project(4, 1, layer)
        attend(1, layer)
        reduce_and_share(0)
        reduce_out(7, 1, layer, 'o', abuf, q_rows)
        shared(0)
        norm(0, gm_ref, layer)
        gate_up(8, layer, 0, a_cut)
        reduce_and_share(1)
        gate_up(8, layer, a_cut, n_f)
        reduce_out(9, 0, layer, 'd', ubuf, ffn)
        shared(1)
        norm(1, gm_ref, layer)
        gate_up(10, layer, 0, b_cut)
        reduce_and_share(0)
        gate_up(10, layer, b_cut, n_f)
        reduce_out(11, 1, layer, 'd', ubuf, ffn)
        return carry

    lax.fori_loop(0, layers, layer_body, 0)
    shared(0)
    first = pltpu.make_async_copy(xbuf.at[pl.ds(0, rows), :], out_hbm.at[pl.ds(0, rows), :], load_sem.at[0])
    first.start()
    reduce_and_share(1)
    shared(1)
    second = pltpu.make_async_copy(xbuf.at[pl.ds(rows, rows), :], out_hbm.at[pl.ds(rows, rows), :], load_sem.at[1])
    second.start()
    first.wait()
    second.wait()


def solution(mesh):
    owners = mesh.shape['pool']

    def local_fn(kv_pool, page_idx, x_tokens, gain_attn, w_q, w_k, w_v, w_o, gain_mlp, w_gate, w_up, w_down):
        layers, pages, _, page_len, kv_loc, head_dim = kv_pool.shape
        tokens, width = x_tokens.shape[1:]
        ffn = w_gate.shape[2]
        req_pages = page_idx.shape[2]
        q_loc = w_q.shape[2] // head_dim
        group_q = q_loc // kv_loc
        prefix = owners * req_pages * page_len
        rows = tokens // 2

        wanted = page_idx.reshape(owners * req_pages)
        wanted = (wanted[None, :] + pages * jnp.arange(layers, dtype=wanted.dtype)[:, None]).reshape(-1)
        flat = kv_pool.reshape(layers * pages, 2, page_len, kv_loc, head_dim)
        picked = jnp.take(flat, wanted, axis=0, mode='clip').reshape(layers, owners, req_pages, 2, page_len, kv_loc, head_dim)
        picked = picked.transpose(1, 0, 3, 5, 2, 4, 6).reshape(owners, layers * 2 * kv_loc, req_pages * page_len, head_dim)
        received = lax.all_to_all(picked, 'pool', 0, 0, tiled=True)
        kv_pre = received.transpose(1, 0, 2, 3).reshape(layers, 2, kv_loc, prefix, head_dim)

        cos_tab, sin_tab = rope_tables(prefix, tokens, head_dim)
        gains = [g.astype(F32).reshape(layers, 1, width) for g in (gain_attn, gain_mlp)]
        hbm = pl.BlockSpec(memory_space=pl.ANY)
        vmem = pl.BlockSpec(memory_space=pltpu.VMEM)
        dims = (layers, tokens, kv_loc, group_q, head_dim, width, ffn, prefix)
        weights = (w_q, w_k, w_v, w_o, w_gate, w_up, w_down)
        n_bytes = 2 * sum(w.size * 2 for w in weights)
        out = pl.pallas_call(
            functools.partial(layers_kernel, dims),
            out_shape=jax.ShapeDtypeStruct((tokens, width), BF16),
            in_specs=[hbm, hbm, vmem, vmem, vmem, vmem] + [hbm] * 7,
            out_specs=hbm,
            scratch_shapes=[
                pltpu.VMEM((SLOTS, max(ffn, width), TILE), BF16),
                pltpu.VMEM((tokens, width), BF16),
                pltpu.VMEM((rows, width), BF16),
                pltpu.VMEM((q_loc, rows, head_dim), BF16),
                pltpu.VMEM((kv_loc, tokens, head_dim), BF16),
                pltpu.VMEM((kv_loc, tokens, head_dim), BF16),
                pltpu.VMEM((rows, q_loc * head_dim), BF16),
                pltpu.VMEM((rows, ffn), BF16),
                pltpu.VMEM((2, rows, width), F32),
                pltpu.VMEM((2, rows // 2, width), F32),
                pltpu.VMEM((layers, 2, kv_loc, prefix, head_dim), BF16),
                pltpu.SemaphoreType.DMA((SLOTS,)),
                pltpu.SemaphoreType.DMA((2,)),
                pltpu.SemaphoreType.DMA((2,)),
                pltpu.SemaphoreType.DMA((2,)),
                pltpu.SemaphoreType.DMA((2,)),
                pltpu.SemaphoreType.DMA((2,)),
            ],
            compiler_params=pltpu.CompilerParams(collective_id=0, has_side_effects=True, vmem_limit_bytes=62 * 1024 * 1024),
            cost_estimate=pl.CostEstimate(flops=tokens * n_bytes // 2, bytes_accessed=n_bytes, transcendentals=0),
        )(kv_pre, x_tokens[0], cos_tab, sin_tab, *gains, *weights)
        return out[None]

    pool_spec = P(None, ('rep', 'pool'), None, None, 'heads', None)
    index_spec = P('rep', 'pool', None)
    x_spec = P(('rep', 'pool'), None, None)
    gain_spec = P(None, None)
    col_spec = P(None, None, 'heads')
    row_spec = P(None, 'heads', None)
    return jax.shard_map(local_fn, mesh=mesh, in_specs=(pool_spec, index_spec, x_spec, gain_spec, col_spec, col_spec, col_spec, row_spec, gain_spec, col_spec, col_spec, row_spec), out_specs=x_spec, check_vma=False)
```

```python
import functools

import jax
import jax.numpy as jnp
from jax import lax
from jax.experimental import pallas as pl
from jax.experimental.pallas import tpu as pltpu
from jax.sharding import PartitionSpec as P

MESH = pl.DeviceIdType.MESH
F32 = jnp.float32
BF16 = jnp.bfloat16
TILE = 256
SLOTS = 9
AHEAD = SLOTS - 1


def rope_tables(prefix, tokens, head_dim):
    positions = (prefix + jnp.arange(tokens)).astype(F32)
    inv_freq = 10000.0 ** (-2.0 * jnp.arange(head_dim // 2).astype(F32) / head_dim)
    angles = positions[:, None] * inv_freq[None, :]
    cos_tab, sin_tab = jnp.cos(angles), jnp.sin(angles)
    return jnp.concatenate([cos_tab, cos_tab], axis=-1), jnp.concatenate([-sin_tab, sin_tab], axis=-1)


def layers_kernel(
    dims,
    kv_hbm, x_hbm, cos_ref, sin_ref, ga_ref, gm_ref,
    wq_hbm, wk_hbm, wv_hbm, wo_hbm, wg_hbm, wu_hbm, wd_hbm,
    out_hbm,
    ring, xbuf, hbuf, qbuf, kbuf, vbuf, abuf, ubuf, pbuf, rbuf, kvbuf,
    ring_sem, load_sem, rs_send, rs_recv, ag_send, ag_recv, kv_send, kv_recv,
):
    layers, tokens, kv_loc, group_q, head_dim, width, ffn, prefix, owners = dims
    q_loc = kv_loc * group_q
    rows = tokens // 2
    half = rows // 2
    per_tile = TILE // head_dim
    scale = head_dim ** -0.5

    me = lax.axis_index('heads')
    other = 1 - me
    pool = lax.axis_index('pool')
    own_len = prefix // owners

    n_q, n_kv = q_loc * head_dim // TILE, kv_loc * head_dim // TILE
    n_d, n_f = width // TILE, ffn // TILE
    attn_seq = [('q', n_q), ('k', n_kv), ('v', n_kv), ('o', n_d)]
    mlp_seq = [('gu', 2 * n_f), ('d', n_d)]
    phases = attn_seq + attn_seq + mlp_seq + mlp_seq
    bases = [sum(n for _, n in phases[:p]) for p in range(len(phases))]
    per_layer = sum(n for _, n in phases)
    q_rows = q_loc * head_dim

    def copies(kind, layer, idx, slot):
        def tile(w_hbm, depth, col):
            start = col * TILE if isinstance(col, int) else pl.multiple_of(col * TILE, TILE)
            return pltpu.make_async_copy(w_hbm.at[layer, :, pl.ds(start, TILE)], ring.at[slot, pl.ds(0, depth), :], ring_sem.at[slot])
        if kind == 'q':
            return tile(wq_hbm, width, idx)
        if kind == 'k':
            return tile(wk_hbm, width, idx)
        if kind == 'v':
            return tile(wv_hbm, width, idx)
        if kind == 'o':
            return tile(wo_hbm, q_rows, idx)
        if kind == 'g':
            return tile(wg_hbm, width, idx)
        if kind == 'u':
            return tile(wu_hbm, width, idx)
        return tile(wd_hbm, ffn, idx)

    def start_tile(phase, layer, idx, slot):
        kind = phases[phase][0]
        if kind != 'gu':
            copies(kind, layer, idx, slot).start()
        elif isinstance(idx, int):
            copies('gu'[idx % 2], layer, idx // 2, slot).start()
        else:
            @pl.when(lax.rem(idx, 2) == 0)
            def _():
                copies('g', layer, idx // 2, slot).start()

            @pl.when(lax.rem(idx, 2) == 1)
            def _():
                copies('u', layer, idx // 2, slot).start()

    def prefetch(phase, layer, idx):
        slot = lax.rem(layer * per_layer + bases[phase] + idx + AHEAD, SLOTS)
        lo = -AHEAD
        p, wrapped = phase, False
        count = phases[phase][1]
        while lo < count:
            hi = lo + phases[p][1]
            if hi > 0:
                local = idx - lo
                cond = (idx >= lo) & (idx < hi)
                target = layer + 1 if wrapped else layer
                if wrapped:
                    cond = cond & (target < layers)

                @pl.when(cond)
                def _(p=p, target=target, local=local):
                    start_tile(p, target, local, slot)
            lo = hi
            p += 1
            if p == len(phases):
                p, wrapped = 0, True

    def take(phase, layer, idx, kind, col):
        prefetch(phase, layer, idx)
        slot = lax.rem(layer * per_layer + bases[phase] + idx, SLOTS)
        copies(kind, layer, col, slot).wait()
        return slot

    def norm(chunk, gain_ref, layer):
        step = 16

        def body(i, carry):
            at = pl.multiple_of(chunk * rows + i * step, step)
            to = pl.multiple_of(i * step, step)
            hid = xbuf[pl.ds(at, step), :].astype(F32)
            inv = lax.rsqrt(jnp.mean(hid * hid, axis=-1, keepdims=True) + 1e-5)
            hbuf[pl.ds(to, step), :] = (hid * inv * gain_ref[layer]).astype(BF16)
            return carry

        lax.fori_loop(0, rows // step, body, 0)

    def roped(block, chunk):
        cos = cos_ref[chunk * rows:(chunk + 1) * rows, :]
        sin = sin_ref[chunk * rows:(chunk + 1) * rows, :]
        return (block * cos + pltpu.roll(block, head_dim // 2, 1) * sin).astype(BF16)

    def project(phase, chunk, layer):
        def q_body(i, carry):
            slot = take(phase, layer, i, 'q', i)
            res = jnp.dot(hbuf[...], ring[slot, :width, :], preferred_element_type=F32)
            for s in range(per_tile):
                qbuf[i * per_tile + s] = roped(res[:, s * head_dim:(s + 1) * head_dim], chunk)
            return carry

        def k_body(i, carry):
            slot = take(phase + 1, layer, i, 'k', i)
            res = jnp.dot(hbuf[...], ring[slot, :width, :], preferred_element_type=F32)
            for s in range(per_tile):
                kbuf[i * per_tile + s, chunk * rows:(chunk + 1) * rows, :] = roped(res[:, s * head_dim:(s + 1) * head_dim], chunk)
            return carry

        def v_body(i, carry):
            slot = take(phase + 2, layer, i, 'v', i)
            res = jnp.dot(hbuf[...], ring[slot, :width, :], preferred_element_type=F32)
            for s in range(per_tile):
                vbuf[i * per_tile + s, chunk * rows:(chunk + 1) * rows, :] = res[:, s * head_dim:(s + 1) * head_dim].astype(BF16)
            return carry

        lax.fori_loop(0, n_q, q_body, 0)
        lax.fori_loop(0, n_kv, k_body, 0)
        lax.fori_loop(0, n_kv, v_body, 0)

    def attend(chunk, layer):
        n_new = (chunk + 1) * rows
        nt = (((1,), (1,)), ((), ()))

        def body(g, carry):
            for r in range(group_q):
                q = qbuf[g * group_q + r]
                s_pre = lax.dot_general(q, kvbuf[layer, g], nt, preferred_element_type=F32) * scale
                s_new = lax.dot_general(q, kbuf[g, :n_new, :], nt, preferred_element_type=F32) * scale
                tok = chunk * rows + lax.broadcasted_iota(jnp.int32, (rows, n_new), 0)
                key = lax.broadcasted_iota(jnp.int32, (rows, n_new), 1)
                s_new = jnp.where(key <= tok, s_new, -jnp.inf)
                top = jnp.maximum(jnp.max(s_pre, axis=-1, keepdims=True), jnp.max(s_new, axis=-1, keepdims=True))
                e_pre = jnp.exp(s_pre - top)
                e_new = jnp.exp(s_new - top)
                inv = 1.0 / (jnp.sum(e_pre, axis=-1, keepdims=True) + jnp.sum(e_new, axis=-1, keepdims=True))
                att = jnp.dot((e_pre * inv).astype(BF16), kvbuf[layer, kv_loc + g], preferred_element_type=F32)
                att = att + jnp.dot((e_new * inv).astype(BF16), vbuf[g, :n_new, :], preferred_element_type=F32)
                col = pl.multiple_of((g * group_q + r) * head_dim, head_dim)
                abuf[:, pl.ds(col, head_dim)] = att.astype(BF16)
            return carry

        lax.fori_loop(0, kv_loc, body, 0)

    def send_block(chunk, col, cols):
        at = pl.multiple_of(other * half, half)
        return pltpu.make_async_remote_copy(
            src_ref=pbuf.at[chunk, pl.ds(at, half), pl.ds(col, cols)],
            dst_ref=rbuf.at[chunk, :, pl.ds(col, cols)],
            send_sem=rs_send.at[chunk],
            recv_sem=rs_recv.at[chunk],
            device_id={'heads': other},
            device_id_type=MESH,
        )

    def reduce_out(phase, chunk, layer, kind, src, depth):
        def body(i, carry):
            slot = take(phase, layer, i, kind, i)
            res = jnp.dot(src[...], ring[slot, :depth, :], preferred_element_type=F32)
            pbuf[chunk, :, pl.ds(pl.multiple_of(i * TILE, TILE), TILE)] = res

            @pl.when(i > 0)
            def _():
                send_block(chunk, pl.multiple_of((i - 1) * TILE, TILE), TILE).start()
            return carry

        lax.fori_loop(0, n_d, body, 0)
        send_block(chunk, width - TILE, TILE).start()

    def share(chunk):
        at = pl.multiple_of(chunk * rows + me * half, half)
        return pltpu.make_async_remote_copy(
            src_ref=xbuf.at[pl.ds(at, half), :],
            dst_ref=xbuf.at[pl.ds(at, half), :],
            send_sem=ag_send.at[chunk],
            recv_sem=ag_recv.at[chunk],
            device_id={'heads': other},
            device_id_type=MESH,
        )

    def reduce_and_share(chunk):
        whole = send_block(chunk, 0, width)
        whole.wait_recv()
        step = 16

        def body(i, carry):
            at = pl.multiple_of(chunk * rows + me * half + i * step, step)
            mine = pl.multiple_of(me * half + i * step, step)
            got = pl.multiple_of(i * step, step)
            total = pbuf[chunk, pl.ds(mine, step), :] + rbuf[chunk, pl.ds(got, step), :]
            xbuf[pl.ds(at, step), :] = (xbuf[pl.ds(at, step), :].astype(F32) + total).astype(BF16)
            return carry

        lax.fori_loop(0, half // step, body, 0)
        whole.wait_send()
        share(chunk).start()

    def shared(chunk):
        share(chunk).wait()

    def gate_up(phase, layer, first, last):
        def body(i, carry):
            slot = take(phase, layer, 2 * i, 'g', i)
            gate = jnp.dot(hbuf[...], ring[slot, :width, :], preferred_element_type=F32)
            slot = take(phase, layer, 2 * i + 1, 'u', i)
            up = jnp.dot(hbuf[...], ring[slot, :width, :], preferred_element_type=F32)
            ubuf[:, pl.ds(pl.multiple_of(i * TILE, TILE), TILE)] = (jax.nn.silu(gate) * up).astype(BF16)
            return carry

        lax.fori_loop(first, last, body, 0)

    def page_place(layer):
        return kvbuf.at[layer, :, pl.ds(pl.multiple_of(pool * own_len, own_len), own_len), :]

    def page_send(layer, step):
        to = lax.rem(pool + step, owners)
        return pltpu.make_async_remote_copy(
            src_ref=kv_hbm.at[layer, to],
            dst_ref=page_place(layer),
            send_sem=kv_send.at[layer, step],
            recv_sem=kv_recv.at[layer, step],
            device_id={'pool': to},
            device_id_type=MESH,
        )

    def page_keep(layer):
        return pltpu.make_async_copy(kv_hbm.at[layer, pool], page_place(layer), kv_send.at[layer, 0])

    def pages_wait(layer):
        page_keep(layer).wait()
        for step in range(1, owners):
            page_send(layer, step).wait()

    for g in range(AHEAD):
        p = max(k for k in range(len(phases)) if bases[k] <= g)
        start_tile(p, 0, g - bases[p], g)
    x_load = pltpu.make_async_copy(x_hbm, xbuf, load_sem.at[0])
    x_load.start()

    barrier = pltpu.get_barrier_semaphore()
    pl.semaphore_signal(barrier, inc=1, device_id={'heads': other}, device_id_type=MESH)
    for step in range(1, owners):
        pl.semaphore_signal(barrier, inc=1, device_id={'pool': lax.rem(pool + step, owners)}, device_id_type=MESH)
    pl.semaphore_wait(barrier, owners)
    for layer in range(layers):
        for step in range(1, owners):
            page_send(layer, step).start()
        page_keep(layer).start()
    x_load.wait()

    a_cut = min(n_f, 20)
    b_cut = min(n_f, 10)

    def layer_body(layer, carry):
        @pl.when(layer > 0)
        def _():
            shared(0)
        norm(0, ga_ref, layer)
        project(0, 0, layer)

        @pl.when(layer > 0)
        def _():
            reduce_and_share(1)
        pages_wait(layer)
        attend(0, layer)
        reduce_out(3, 0, layer, 'o', abuf, q_rows)

        @pl.when(layer > 0)
        def _():
            shared(1)
        norm(1, ga_ref, layer)
        project(4, 1, layer)
        attend(1, layer)
        reduce_and_share(0)
        reduce_out(7, 1, layer, 'o', abuf, q_rows)
        shared(0)
        norm(0, gm_ref, layer)
        gate_up(8, layer, 0, a_cut)
        reduce_and_share(1)
        gate_up(8, layer, a_cut, n_f)
        reduce_out(9, 0, layer, 'd', ubuf, ffn)
        shared(1)
        norm(1, gm_ref, layer)
        gate_up(10, layer, 0, b_cut)
        reduce_and_share(0)
        gate_up(10, layer, b_cut, n_f)
        reduce_out(11, 1, layer, 'd', ubuf, ffn)
        return carry

    lax.fori_loop(0, layers, layer_body, 0)
    shared(0)
    first = pltpu.make_async_copy(xbuf.at[pl.ds(0, rows), :], out_hbm.at[pl.ds(0, rows), :], load_sem.at[0])
    first.start()
    reduce_and_share(1)
    shared(1)
    second = pltpu.make_async_copy(xbuf.at[pl.ds(rows, rows), :], out_hbm.at[pl.ds(rows, rows), :], load_sem.at[1])
    second.start()
    first.wait()
    second.wait()


def pick_kernel(idx_ref, pool_hbm, out_ref, sems):
    layers, wanted = out_ref.shape[:2]

    def page(layer, i):
        return pltpu.make_async_copy(pool_hbm.at[layer, idx_ref[i]], out_ref.at[layer, i], sems.at[layer, i])

    for layer in range(layers):
        for i in range(wanted):
            page(layer, i).start()
    for layer in range(layers):
        for i in range(wanted):
            page(layer, i).wait()


def solution(mesh):
    owners = mesh.shape['pool']

    def local_fn(kv_pool, page_idx, x_tokens, gain_attn, w_q, w_k, w_v, w_o, gain_mlp, w_gate, w_up, w_down):
        layers, pages, _, page_len, kv_loc, head_dim = kv_pool.shape
        tokens, width = x_tokens.shape[1:]
        ffn = w_gate.shape[2]
        req_pages = page_idx.shape[2]
        q_loc = w_q.shape[2] // head_dim
        group_q = q_loc // kv_loc
        prefix = owners * req_pages * page_len
        rows = tokens // 2

        wanted = page_idx.reshape(owners * req_pages)
        picked = pl.pallas_call(
            pick_kernel,
            out_shape=jax.ShapeDtypeStruct((layers, owners * req_pages) + kv_pool.shape[2:], BF16),
            in_specs=[pl.BlockSpec(memory_space=pltpu.SMEM), pl.BlockSpec(memory_space=pl.ANY)],
            out_specs=pl.BlockSpec(memory_space=pltpu.VMEM),
            scratch_shapes=[pltpu.SemaphoreType.DMA((layers, owners * req_pages))],
        )(wanted, kv_pool)
        picked = picked.reshape(layers, owners, req_pages, 2, page_len, kv_loc, head_dim)
        kv_pre = picked.transpose(0, 1, 3, 5, 2, 4, 6).reshape(layers, owners, 2 * kv_loc, req_pages * page_len, head_dim)

        cos_tab, sin_tab = rope_tables(prefix, tokens, head_dim)
        gains = [g.astype(F32).reshape(layers, 1, width) for g in (gain_attn, gain_mlp)]
        hbm = pl.BlockSpec(memory_space=pl.ANY)
        vmem = pl.BlockSpec(memory_space=pltpu.VMEM)
        dims = (layers, tokens, kv_loc, group_q, head_dim, width, ffn, prefix, owners)
        weights = (w_q, w_k, w_v, w_o, w_gate, w_up, w_down)
        n_bytes = 2 * sum(w.size * 2 for w in weights)
        out = pl.pallas_call(
            functools.partial(layers_kernel, dims),
            out_shape=jax.ShapeDtypeStruct((tokens, width), BF16),
            in_specs=[hbm, hbm, vmem, vmem, vmem, vmem] + [hbm] * 7,
            out_specs=hbm,
            scratch_shapes=[
                pltpu.VMEM((SLOTS, max(ffn, width), TILE), BF16),
                pltpu.VMEM((tokens, width), BF16),
                pltpu.VMEM((rows, width), BF16),
                pltpu.VMEM((q_loc, rows, head_dim), BF16),
                pltpu.VMEM((kv_loc, tokens, head_dim), BF16),
                pltpu.VMEM((kv_loc, tokens, head_dim), BF16),
                pltpu.VMEM((rows, q_loc * head_dim), BF16),
                pltpu.VMEM((rows, ffn), BF16),
                pltpu.VMEM((2, rows, width), F32),
                pltpu.VMEM((2, rows // 2, width), F32),
                pltpu.VMEM((layers, 2 * kv_loc, prefix, head_dim), BF16),
                pltpu.SemaphoreType.DMA((SLOTS,)),
                pltpu.SemaphoreType.DMA((2,)),
                pltpu.SemaphoreType.DMA((2,)),
                pltpu.SemaphoreType.DMA((2,)),
                pltpu.SemaphoreType.DMA((2,)),
                pltpu.SemaphoreType.DMA((2,)),
                pltpu.SemaphoreType.DMA((layers, owners)),
                pltpu.SemaphoreType.DMA((layers, owners)),
            ],
            compiler_params=pltpu.CompilerParams(collective_id=0, has_side_effects=True, vmem_limit_bytes=62 * 1024 * 1024),
            cost_estimate=pl.CostEstimate(flops=tokens * n_bytes // 2, bytes_accessed=n_bytes, transcendentals=0),
        )(kv_pre, x_tokens[0], cos_tab, sin_tab, *gains, *weights)
        return out[None]

    pool_spec = P(None, ('rep', 'pool'), None, None, 'heads', None)
    index_spec = P('rep', 'pool', None)
    x_spec = P(('rep', 'pool'), None, None)
    gain_spec = P(None, None)
    col_spec = P(None, None, 'heads')
    row_spec = P(None, 'heads', None)
    return jax.shard_map(local_fn, mesh=mesh, in_specs=(pool_spec, index_spec, x_spec, gain_spec, col_spec, col_spec, col_spec, row_spec, gain_spec, col_spec, col_spec, row_spec), out_specs=x_spec, check_vma=False)
```

```python
import functools

import jax
import jax.numpy as jnp
import numpy as np
from jax import lax
from jax.experimental import pallas as pl
from jax.experimental.pallas import tpu as pltpu
from jax.sharding import PartitionSpec as P

MESH = pl.DeviceIdType.MESH
F32 = jnp.float32
BF16 = jnp.bfloat16
TILE = 256
SLOTS = 9
PIECE = 1
AHEAD = SLOTS - 1


def rope_tables(prefix, tokens, head_dim):
    positions = (prefix + np.arange(tokens)).astype(np.float32)
    inv_freq = np.float32(10000.0) ** (np.float32(-2.0) * np.arange(head_dim // 2).astype(np.float32) / np.float32(head_dim))
    angles = (positions[:, None] * inv_freq[None, :]).astype(np.float32)
    cos_tab, sin_tab = np.cos(angles), np.sin(angles)
    cos_tab = np.concatenate([cos_tab, cos_tab], axis=-1).astype(np.float32)
    sin_tab = np.concatenate([-sin_tab, sin_tab], axis=-1).astype(np.float32)
    return jnp.asarray(cos_tab), jnp.asarray(sin_tab)


def layers_kernel(
    dims,
    kv_hbm, x_hbm, cos_ref, sin_ref, ga_in, gm_in,
    wq_hbm, wk_hbm, wv_hbm, wo_hbm, wg_hbm, wu_hbm, wd_hbm,
    out_hbm,
    ga_ref, gm_ref, ring, xbuf, hbuf, qbuf, kbuf, vbuf, abuf, ubuf, pbuf, rbuf, kvbuf,
    ring_sem, load_sem, rs_send, rs_recv, ag_send, ag_recv, kv_send, kv_recv,
):
    layers, tokens, kv_loc, group_q, head_dim, width, ffn, prefix, owners = dims
    q_loc = kv_loc * group_q
    rows = tokens // 2
    half = rows // 2
    per_tile = TILE // head_dim
    scale = head_dim ** -0.5

    me = lax.axis_index('heads')
    other = 1 - me
    pool = lax.axis_index('pool')
    own_len = prefix // owners

    n_q, n_kv = q_loc * head_dim // TILE, kv_loc * head_dim // TILE
    n_d, n_f = width // TILE, ffn // TILE
    attn_seq = [('q', n_q), ('k', n_kv), ('v', n_kv), ('o', n_d)]
    mlp_seq = [('gu', 2 * n_f), ('d', n_d)]
    phases = attn_seq + attn_seq + mlp_seq + mlp_seq
    bases = [sum(n for _, n in phases[:p]) for p in range(len(phases))]
    per_layer = sum(n for _, n in phases)
    q_rows = q_loc * head_dim
    cols = width // 2

    def copies(kind, layer, idx, slot):
        def tile(w_hbm, depth, col):
            start = col * TILE if isinstance(col, int) else pl.multiple_of(col * TILE, TILE)
            return pltpu.make_async_copy(w_hbm.at[layer, :, pl.ds(start, TILE)], ring.at[slot, pl.ds(0, depth), :], ring_sem.at[slot])
        if kind == 'q':
            return tile(wq_hbm, width, idx)
        if kind == 'k':
            return tile(wk_hbm, width, idx)
        if kind == 'v':
            return tile(wv_hbm, width, idx)
        if kind == 'o':
            return tile(wo_hbm, q_rows, idx)
        if kind == 'g':
            return tile(wg_hbm, width, idx)
        if kind == 'u':
            return tile(wu_hbm, width, idx)
        return tile(wd_hbm, ffn, idx)

    def start_tile(phase, layer, idx, slot):
        kind = phases[phase][0]
        if kind != 'gu':
            copies(kind, layer, idx, slot).start()
        elif isinstance(idx, int):
            copies('gu'[idx % 2], layer, idx // 2, slot).start()
        else:
            for part in range(2):
                @pl.when(lax.rem(idx, 2) == part)
                def _(part=part):
                    copies('gu'[part], layer, idx // 2, slot).start()

    def prefetch(phase, layer, idx):
        slot = lax.rem(layer * per_layer + bases[phase] + idx + AHEAD, SLOTS)
        lo = -AHEAD
        p, wrapped = phase, False
        count = phases[phase][1]
        while lo < count:
            hi = lo + phases[p][1]
            if hi > 0:
                local = idx - lo
                cond = (idx >= lo) & (idx < hi)
                target = layer + 1 if wrapped else layer
                if wrapped:
                    cond = cond & (target < layers)

                @pl.when(cond)
                def _(p=p, target=target, local=local):
                    start_tile(p, target, local, slot)
            lo = hi
            p += 1
            if p == len(phases):
                p, wrapped = 0, True

    def take(phase, layer, idx, kind, col):
        prefetch(phase, layer, idx)
        slot = lax.rem(layer * per_layer + bases[phase] + idx, SLOTS)
        copies(kind, layer, col, slot).wait()
        return slot

    def norm(chunk, gain_ref, layer):
        step = 16

        def body(i, carry):
            at = pl.multiple_of(chunk * rows + i * step, step)
            to = pl.multiple_of(i * step, step)
            hid = xbuf[pl.ds(at, step), :].astype(F32)
            inv = lax.rsqrt(jnp.mean(hid * hid, axis=-1, keepdims=True) + 1e-5)
            hbuf[pl.ds(to, step), :] = (hid * inv * gain_ref[layer]).astype(BF16)
            return carry

        lax.fori_loop(0, rows // step, body, 0)

    def roped(block, chunk):
        cos = cos_ref[chunk * rows:(chunk + 1) * rows, :]
        sin = sin_ref[chunk * rows:(chunk + 1) * rows, :]
        return (block * cos + pltpu.roll(block, head_dim // 2, 1) * sin).astype(BF16)

    def project(phase, chunk, layer):
        def q_body(i, carry):
            slot = take(phase, layer, i, 'q', i)
            res = jnp.dot(hbuf[...], ring[slot, :width, :], preferred_element_type=F32)
            for s in range(per_tile):
                qbuf[i * per_tile + s] = roped(res[:, s * head_dim:(s + 1) * head_dim], chunk)
            return carry

        def k_body(i, carry):
            slot = take(phase + 1, layer, i, 'k', i)
            res = jnp.dot(hbuf[...], ring[slot, :width, :], preferred_element_type=F32)
            for s in range(per_tile):
                kbuf[i * per_tile + s, chunk * rows:(chunk + 1) * rows, :] = roped(res[:, s * head_dim:(s + 1) * head_dim], chunk)
            return carry

        def v_body(i, carry):
            slot = take(phase + 2, layer, i, 'v', i)
            res = jnp.dot(hbuf[...], ring[slot, :width, :], preferred_element_type=F32)
            for s in range(per_tile):
                vbuf[i * per_tile + s, chunk * rows:(chunk + 1) * rows, :] = res[:, s * head_dim:(s + 1) * head_dim].astype(BF16)
            return carry

        lax.fori_loop(0, n_q, q_body, 0)
        lax.fori_loop(0, n_kv, k_body, 0)
        lax.fori_loop(0, n_kv, v_body, 0)

    def attend(chunk, layer):
        n_new = (chunk + 1) * rows
        nt = (((1,), (1,)), ((), ()))

        def body(g, carry):
            for r in range(group_q):
                q = qbuf[g * group_q + r]
                s_pre = lax.dot_general(q, kvbuf[layer, g], nt, preferred_element_type=F32) * scale
                s_new = lax.dot_general(q, kbuf[g, :n_new, :], nt, preferred_element_type=F32) * scale
                tok = chunk * rows + lax.broadcasted_iota(jnp.int32, (rows, n_new), 0)
                key = lax.broadcasted_iota(jnp.int32, (rows, n_new), 1)
                s_new = jnp.where(key <= tok, s_new, -jnp.inf)
                top = jnp.maximum(jnp.max(s_pre, axis=-1, keepdims=True), jnp.max(s_new, axis=-1, keepdims=True))
                e_pre = jnp.exp(s_pre - top)
                e_new = jnp.exp(s_new - top)
                inv = 1.0 / (jnp.sum(e_pre, axis=-1, keepdims=True) + jnp.sum(e_new, axis=-1, keepdims=True))
                att = jnp.dot((e_pre * inv).astype(BF16), kvbuf[layer, kv_loc + g], preferred_element_type=F32)
                att = att + jnp.dot((e_new * inv).astype(BF16), vbuf[g, :n_new, :], preferred_element_type=F32)
                col = pl.multiple_of((g * group_q + r) * head_dim, head_dim)
                abuf[:, pl.ds(col, head_dim)] = att.astype(BF16)
            return carry

        lax.fori_loop(0, kv_loc, body, 0)

    def send_block(chunk, part, col, n_cols):
        at = pl.multiple_of(other * half, half)
        return pltpu.make_async_remote_copy(
            src_ref=pbuf.at[chunk, pl.ds(at, half), pl.ds(col, n_cols)],
            dst_ref=rbuf.at[chunk, :, pl.ds(col, n_cols)],
            send_sem=rs_send.at[chunk, part],
            recv_sem=rs_recv.at[chunk, part],
            device_id={'heads': other},
            device_id_type=MESH,
        )

    piece = PIECE * TILE

    def reduce_out(phase, chunk, layer):
        kind = phases[phase][0]
        src, depth = (ubuf, ffn) if kind == 'd' else (abuf, q_rows)

        def body(i, carry):
            slot = take(phase, layer, i, kind, i)
            res = jnp.dot(src[...], ring[slot, :depth, :], preferred_element_type=F32)
            pbuf[chunk, :, pl.ds(pl.multiple_of(i * TILE, TILE), TILE)] = res

            @pl.when((i > 0) & (lax.rem(i, PIECE) == 0))
            def _():
                col = pl.multiple_of((i - PIECE) * TILE, TILE)

                @pl.when(i * TILE <= cols)
                def _():
                    send_block(chunk, 0, col, piece).start()

                @pl.when(i * TILE > cols)
                def _():
                    send_block(chunk, 1, col, piece).start()
            return carry

        lax.fori_loop(0, n_d, body, 0)
        send_block(chunk, 1, width - piece, piece).start()

    def share(chunk, part):
        at = pl.multiple_of(chunk * rows + me * half, half)
        place = xbuf.at[pl.ds(at, half), pl.ds(part * cols, cols)]
        return pltpu.make_async_remote_copy(
            src_ref=place,
            dst_ref=place,
            send_sem=ag_send.at[chunk, part],
            recv_sem=ag_recv.at[chunk, part],
            device_id={'heads': other},
            device_id_type=MESH,
        )

    def reduce_and_share(chunk, part):
        whole = send_block(chunk, part, part * cols, cols)
        whole.wait_recv()
        step = 16
        side = slice(part * cols, (part + 1) * cols)

        def body(i, carry):
            at = pl.multiple_of(chunk * rows + me * half + i * step, step)
            mine = pl.multiple_of(me * half + i * step, step)
            got = pl.multiple_of(i * step, step)
            total = pbuf[chunk, pl.ds(mine, step), side] + rbuf[chunk, pl.ds(got, step), side]
            xbuf[pl.ds(at, step), side] = (xbuf[pl.ds(at, step), side].astype(F32) + total).astype(BF16)
            return carry

        lax.fori_loop(0, half // step, body, 0)
        whole.wait_send()
        share(chunk, part).start()

    def shared(chunk):
        share(chunk, 0).wait()
        share(chunk, 1).wait()

    def gate_up(phase, layer, first, last):
        def body(i, carry):
            slot = take(phase, layer, 2 * i, 'g', i)
            gate = jnp.dot(hbuf[...], ring[slot, :width, :], preferred_element_type=F32)
            slot = take(phase, layer, 2 * i + 1, 'u', i)
            up = jnp.dot(hbuf[...], ring[slot, :width, :], preferred_element_type=F32)
            ubuf[:, pl.ds(pl.multiple_of(i * TILE, TILE), TILE)] = (jax.nn.silu(gate) * up).astype(BF16)
            return carry

        lax.fori_loop(first, last, body, 0)

    def page_place(layer):
        return kvbuf.at[layer, :, pl.ds(pl.multiple_of(pool * own_len, own_len), own_len), :]

    def page_send(layer, step):
        to = lax.rem(pool + step, owners)
        return pltpu.make_async_remote_copy(
            src_ref=kv_hbm.at[layer, to],
            dst_ref=page_place(layer),
            send_sem=kv_send.at[layer, step],
            recv_sem=kv_recv.at[layer, step],
            device_id={'pool': to},
            device_id_type=MESH,
        )

    def page_keep(layer):
        return pltpu.make_async_copy(kv_hbm.at[layer, pool], page_place(layer), kv_send.at[layer, 0])

    def pages_wait(layer):
        page_keep(layer).wait()
        for step in range(1, owners):
            page_send(layer, step).wait()

    for g in range(AHEAD):
        p = max(k for k in range(len(phases)) if bases[k] <= g)
        start_tile(p, 0, g - bases[p], g)
    x_load = pltpu.make_async_copy(x_hbm, xbuf, load_sem.at[0])
    x_load.start()

    barrier = pltpu.get_barrier_semaphore()
    pl.semaphore_signal(barrier, inc=1, device_id={'heads': other}, device_id_type=MESH)
    for step in range(1, owners):
        pl.semaphore_signal(barrier, inc=1, device_id={'pool': lax.rem(pool + step, owners)}, device_id_type=MESH)
    pl.semaphore_wait(barrier, owners)
    for layer in range(layers):
        for step in range(1, owners):
            page_send(layer, step).start()
        page_keep(layer).start()
    for layer in range(layers):
        ga_ref[layer] = ga_in[layer:layer + 1, :].astype(F32)
        gm_ref[layer] = gm_in[layer:layer + 1, :].astype(F32)
    x_load.wait()

    a_cut = min(n_f, 20)
    b_cut = min(n_f, 10)

    def served_gate_up(phase, layer, cut, chunk):
        gate_up(phase, layer, 0, cut)
        reduce_and_share(chunk, 0)
        reduce_and_share(chunk, 1)
        gate_up(phase, layer, cut, n_f)

    def layer_body(layer, carry):
        def serve(part):
            @pl.when(layer > 0)
            def _():
                reduce_and_share(1, part)

        @pl.when(layer > 0)
        def _():
            shared(0)
        norm(0, ga_ref, layer)
        project(0, 0, layer)
        serve(0)
        serve(1)
        pages_wait(layer)
        attend(0, layer)
        reduce_out(3, 0, layer)

        @pl.when(layer > 0)
        def _():
            shared(1)
        norm(1, ga_ref, layer)
        project(4, 1, layer)
        attend(1, layer)
        reduce_and_share(0, 0)
        reduce_and_share(0, 1)
        reduce_out(7, 1, layer)
        shared(0)
        norm(0, gm_ref, layer)
        served_gate_up(8, layer, a_cut, 1)
        reduce_out(9, 0, layer)
        shared(1)
        norm(1, gm_ref, layer)
        served_gate_up(10, layer, b_cut, 0)
        reduce_out(11, 1, layer)
        return carry

    lax.fori_loop(0, layers, layer_body, 0)
    shared(0)
    first = pltpu.make_async_copy(xbuf.at[pl.ds(0, rows), :], out_hbm.at[pl.ds(0, rows), :], load_sem.at[0])
    first.start()
    reduce_and_share(1, 0)
    reduce_and_share(1, 1)
    shared(1)
    second = pltpu.make_async_copy(xbuf.at[pl.ds(rows, rows), :], out_hbm.at[pl.ds(rows, rows), :], load_sem.at[1])
    second.start()
    first.wait()
    second.wait()


def pick_kernel(idx_ref, pool_hbm, out_ref, sems):
    layers, wanted = out_ref.shape[:2]
    req_pages = idx_ref.shape[2]

    def page(layer, i):
        return pltpu.make_async_copy(pool_hbm.at[layer, idx_ref[i // req_pages, 0, i % req_pages]], out_ref.at[layer, i], sems.at[layer, i])

    for layer in range(layers):
        for i in range(wanted):
            page(layer, i).start()
    for layer in range(layers):
        for i in range(wanted):
            page(layer, i).wait()


def solution(mesh):
    owners = mesh.shape['pool']

    def local_fn(kv_pool, page_idx, x_tokens, gain_attn, w_q, w_k, w_v, w_o, gain_mlp, w_gate, w_up, w_down):
        layers, pages, _, page_len, kv_loc, head_dim = kv_pool.shape
        tokens, width = x_tokens.shape[1:]
        ffn = w_gate.shape[2]
        req_pages = page_idx.shape[2]
        q_loc = w_q.shape[2] // head_dim
        group_q = q_loc // kv_loc
        prefix = owners * req_pages * page_len
        rows = tokens // 2

        picked = pl.pallas_call(
            pick_kernel,
            out_shape=jax.ShapeDtypeStruct((layers, owners * req_pages) + kv_pool.shape[2:], BF16),
            in_specs=[pl.BlockSpec(memory_space=pltpu.SMEM), pl.BlockSpec(memory_space=pl.ANY)],
            out_specs=pl.BlockSpec(memory_space=pltpu.VMEM),
            scratch_shapes=[pltpu.SemaphoreType.DMA((layers, owners * req_pages))],
        )(page_idx, kv_pool)
        picked = picked.reshape(layers, owners, req_pages, 2, page_len, kv_loc, head_dim)
        kv_pre = picked.transpose(0, 1, 3, 5, 2, 4, 6).reshape(layers, owners, 2 * kv_loc, req_pages * page_len, head_dim)

        cos_tab, sin_tab = rope_tables(prefix, tokens, head_dim)
        hbm = pl.BlockSpec(memory_space=pl.ANY)
        vmem = pl.BlockSpec(memory_space=pltpu.VMEM)
        dims = (layers, tokens, kv_loc, group_q, head_dim, width, ffn, prefix, owners)
        weights = (w_q, w_k, w_v, w_o, w_gate, w_up, w_down)
        n_bytes = 2 * sum(w.size * 2 for w in weights)
        out = pl.pallas_call(
            functools.partial(layers_kernel, dims),
            out_shape=jax.ShapeDtypeStruct((tokens, width), BF16),
            in_specs=[hbm, hbm, vmem, vmem, vmem, vmem] + [hbm] * 7,
            out_specs=hbm,
            scratch_shapes=[
                pltpu.VMEM((layers, 1, width), F32),
                pltpu.VMEM((layers, 1, width), F32),
                pltpu.VMEM((SLOTS, max(ffn, width), TILE), BF16),
                pltpu.VMEM((tokens, width), BF16),
                pltpu.VMEM((rows, width), BF16),
                pltpu.VMEM((q_loc, rows, head_dim), BF16),
                pltpu.VMEM((kv_loc, tokens, head_dim), BF16),
                pltpu.VMEM((kv_loc, tokens, head_dim), BF16),
                pltpu.VMEM((rows, q_loc * head_dim), BF16),
                pltpu.VMEM((rows, ffn), BF16),
                pltpu.VMEM((2, rows, width), F32),
                pltpu.VMEM((2, rows // 2, width), F32),
                pltpu.VMEM((layers, 2 * kv_loc, prefix, head_dim), BF16),
                pltpu.SemaphoreType.DMA((SLOTS,)),
                pltpu.SemaphoreType.DMA((2,)),
                pltpu.SemaphoreType.DMA((2, 2)),
                pltpu.SemaphoreType.DMA((2, 2)),
                pltpu.SemaphoreType.DMA((2, 2)),
                pltpu.SemaphoreType.DMA((2, 2)),
                pltpu.SemaphoreType.DMA((layers, owners)),
                pltpu.SemaphoreType.DMA((layers, owners)),
            ],
            compiler_params=pltpu.CompilerParams(collective_id=0, has_side_effects=True, vmem_limit_bytes=62 * 1024 * 1024),
            cost_estimate=pl.CostEstimate(flops=tokens * n_bytes // 2, bytes_accessed=n_bytes, transcendentals=0),
        )(kv_pre, x_tokens[0], cos_tab, sin_tab, gain_attn, gain_mlp, *weights)
        return out[None]

    pool_spec = P(None, ('rep', 'pool'), None, None, 'heads', None)
    index_spec = P('rep', 'pool', None)
    x_spec = P(('rep', 'pool'), None, None)
    gain_spec = P(None, None)
    col_spec = P(None, None, 'heads')
    row_spec = P(None, 'heads', None)
    return jax.shard_map(local_fn, mesh=mesh, in_specs=(pool_spec, index_spec, x_spec, gain_spec, col_spec, col_spec, col_spec, row_spec, gain_spec, col_spec, col_spec, row_spec), out_specs=x_spec, check_vma=False)
```
